32 devices in a mesh: groups: 2 (over y), tensor: 4 (over z), seq: 4 (over x, core).
Axes of the slice: x: 2, y: 2, z: 4, core: 2. Of those that a mesh axis runs over, the one named last changes fastest.
Arguments:
- stream: bfloat16 [2048, 4096], P(('groups', 'seq'), 'tensor'), parts along dimension 0, may hold values from -150 to 150, as said below
- ffn_gain: float32 [4096], replicated, may hold values from 0.5 to 1.5
- final_gain: float32 [4096], replicated, may hold values from 0.5 to 1.5
- w_gate: bfloat16 [4096, 5120], P(None, 'tensor'), may hold values from -0.09375 to 0.09375
- w_up: bfloat16 [4096, 5120], P(None, 'tensor'), may hold values from -0.09375 to 0.09375
- w_out: bfloat16 [5120, 4096], P('tensor'), may hold values from -0.25 to 0.25
- w_key: bfloat16 [4096, 2048], P(None, 'tensor'), may hold values from -0.09375 to 0.09375
- w_value: bfloat16 [4096, 2048], P(None, 'tensor'), may hold values from -0.09375 to 0.09375
Outputs:
- enc_out: bfloat16 [2048, 4096], P(('groups', 'seq'), 'tensor'), parts along dimension 0
- cross_keys: bfloat16 [2048, 2048], P('groups', 'tensor'), parts along dimension 0
- cross_values: bfloat16 [2048, 2048], P('groups', 'tensor'), parts along dimension 0
The draws below stay inside these ranges and needn't reach their ends.
There are 2 independent parts, one for each index of `groups`. The reference program is written for one: setup_inputs(seed, part) draws one part's arguments, and reference() takes and returns one part's arrays. A program takes and returns all parts, laid end to end along the dimension named above; an argument that names none is the same for every part. Nothing has to cross between parts.
Inputs may be any that keep to these rules, and one draw needn't show every extreme that they name: Finite entries of the residual stream.
All inputs are finite; a program needn't handle non-finite values.
Results may differ from the reference program's by a relative error of at most 0.0055.
Values may be sent and summed in bfloat16 or wider, within the bound.
A program may use at most 128 MiB of HBM per device.

```python
import jax
import jax.numpy as jnp
from jax import lax

D = 4096
FF = 5120
TOKENS = 1024
KV_WIDTH = 2048


def draw_stream(key, part):
    key_base = jax.random.fold_in(key, 11)
    key_rows = jax.random.fold_in(key, 12)
    key_cols = jax.random.fold_in(key, 13)
    row_scale = jnp.exp(jax.random.uniform(key_rows, (TOKENS, 1), jnp.float32, jnp.log(0.3), jnp.log(3.0)))
    rising = 3.0 ** (jnp.arange(D, dtype=jnp.float32) / D)
    col_scale = rising[None, :] * jnp.exp(jax.random.uniform(key_cols, (1, D), jnp.float32, 0.0, jnp.log(3.3)))
    base_vals = jax.random.normal(key_base, (TOKENS, D), jnp.float32)
    base_vals = jnp.clip(base_vals, -5.0, 5.0)
    return (base_vals * row_scale * col_scale).astype(jnp.bfloat16)


def strengthened(drawn, own_key, source, target, shards_of, factor):
    def block_of(dim):
        return (jnp.arange(drawn.shape[dim]) // (drawn.shape[dim] // shards_of)).reshape((-1,) + (1,) * (drawn.ndim - 1 - dim))

    one_side = jax.random.permutation(own_key, shards_of)[block_of(target)]
    second = (block_of(target) + shards_of // 2) % shards_of
    return jnp.where((block_of(source) == one_side) | (block_of(source) == second), factor * drawn, drawn)


def shard_levels(key, dims, split, least, largest):
    loudness = 1.0
    for dim, parts in split:
        steps = jax.random.uniform(jax.random.fold_in(jax.random.fold_in(key, 6), dim), (parts,), jnp.float32, least / len(split), largest / len(split))
        loudness = loudness * jnp.repeat(jnp.exp(steps), dims[dim] // parts).reshape((-1,) + (1,) * (len(dims) - 1 - dim))
    return loudness


def gaussian(stream_key, shape, deviation, most, cuts=(), held_as=jnp.bfloat16):
    loudness = shard_levels(stream_key, shape, cuts, -0.22, 0.18) if cuts else 1.0
    drawn = jax.random.normal(stream_key, shape, jnp.float32) * deviation * loudness
    return jnp.minimum(jnp.maximum(drawn, -most), most).astype(held_as)


def noise_with(key, extent, scale, bound, cuts, heavy, held_as=jnp.bfloat16):
    values = scale * jax.random.normal(key, extent, jnp.float32)
    if cuts:
        values = values * shard_levels(key, extent, cuts, -0.22, 0.18)
    return jnp.clip(strengthened(values, jax.random.fold_in(key, 3), *heavy), -bound, bound).astype(held_as)


def setup_inputs(seed: int = 0, part: int = 0) -> dict:
    key_list = jax.random.split(jax.random.key(seed), 9)
    own_keys = jax.random.split(jax.random.fold_in(key_list[8], part), 9)
    return {
        "stream": draw_stream(jax.random.fold_in(jax.random.fold_in(key_list[8], part), 71), part),
        "ffn_gain": jnp.clip(1.0 + 0.1 * jax.random.normal(key_list[1], (D,), jnp.float32), 0.5, 1.5),
        "final_gain": jnp.clip(1.0 + 0.1 * jax.random.normal(key_list[2], (D,), jnp.float32), 0.5, 1.5),
        "w_gate": gaussian(key_list[3], (D, FF), D ** -0.5, 0.09375, ((1, 4),)),
        "w_up": gaussian(key_list[4], (D, FF), D ** -0.5, 0.09375, ((1, 4),)),
        "w_out": noise_with(key_list[5], (FF, D), (FF // 4) ** -0.5, 0.25, ((0, 4),), (0, 1, 4, 2.0)),
        "w_key": gaussian(key_list[6], (D, KV_WIDTH), D ** -0.5, 0.09375, ((1, 4),)),
        "w_value": gaussian(key_list[7], (D, KV_WIDTH), D ** -0.5, 0.09375, ((1, 4),)),
    }


epsilon = 1e-06

def rms_norm(vector, gain):
    return vector * lax.rsqrt(lax.optimization_barrier(jnp.mean(vector * vector, axis=-1, keepdims=True)) + epsilon) * gain

def reference(stream, ffn_gain, final_gain, w_gate, w_up, w_out, w_key, w_value):
    stream_wide = stream.astype(jnp.float32)
    normed_in = rms_norm(stream_wide, ffn_gain).astype(jnp.bfloat16)
    gate_act = jnp.dot(normed_in, w_gate, preferred_element_type=jnp.float32)
    up_proj = jnp.dot(normed_in, w_up, preferred_element_type=jnp.float32)
    hidden = (jax.nn.gelu(gate_act, approximate=True) * up_proj).astype(jnp.bfloat16)
    mixed = stream_wide + jnp.dot(hidden, w_out, preferred_element_type=jnp.float32)
    enc_out = rms_norm(mixed, final_gain).astype(jnp.bfloat16)
    cross_keys = jnp.dot(enc_out, w_key, preferred_element_type=jnp.float32).astype(jnp.bfloat16)
    cross_values = jnp.dot(enc_out, w_value, preferred_element_type=jnp.float32).astype(jnp.bfloat16)
    return (enc_out, cross_keys, cross_values)
```

```python
import functools

import jax
import jax.numpy as jnp
from jax import lax
from jax.experimental import pallas as pl
from jax.experimental.pallas import tpu as pltpu
from jax.sharding import PartitionSpec as P

epsilon = 1e-06
MESH = pl.DeviceIdType.MESH
CHUNKS = 2
SUBS = 2


def block_kernel(
    n, m,
    x_hbm, fg_ref, eg_ref, wg_hbm, wu_hbm, wo_hbm, wk_hbm, wv_hbm,
    enc_hbm, key_hbm, val_hbm,
    wg, wu, wo, wk, wv,
    xs, ms, sent, from_left, from_right,
    gate, up, hid, part, mixed, ssq, kacc, vacc, rsq, enc, kv,
    wsem, xsem, a1s, a1r, rss, rsr, a2s, a2r, sqs, sqr, kvs, kvr, osem,
):
    t = lax.axis_index("tensor")
    s = lax.axis_index("seq")
    _, rows, feat = xs.shape
    crow = rows // CHUNKS
    srow = crow // SUBS
    width = n * feat
    partner = s + 1 - 2 * lax.rem(s, 2)
    mates = [lax.rem(s + 2 * d, m) for d in range(1, m // 2)]
    peers = [lax.rem(t + d, n) for d in range(1, n)]

    def fblk(j):
        return pl.ds(pl.multiple_of(j * feat, feat), feat)

    def x_copy(c):
        r = pl.ds(c * crow, crow)
        return pltpu.make_async_copy(x_hbm.at[r], xs.at[t, r], xsem.at[c])

    def w_in(i, src, dst, j):
        return pltpu.make_async_copy(src.at[fblk(j)], dst.at[fblk(j)], wsem.at[i, j])

    wo_copy = pltpu.make_async_copy(wo_hbm, wo, wsem.at[4, 0])
    for c in range(CHUNKS):
        x_copy(c).start()

    def first_weights(d, carry):
        j = lax.rem(t + d, n)
        w_in(0, wg_hbm, wg, j).start()
        w_in(1, wu_hbm, wu, j).start()
        return carry

    def last_weights(d, carry):
        w_in(2, wk_hbm, wk, d).start()
        w_in(3, wv_hbm, wv, d).start()
        return carry

    lax.fori_loop(0, n, first_weights, 0)
    wo_copy.start()
    lax.fori_loop(0, n, last_weights, 0)

    barrier = pltpu.get_barrier_semaphore()
    for p in peers:
        pl.semaphore_signal(barrier, inc=1, device_id={"tensor": p}, device_id_type=MESH)
    for q in mates + [partner]:
        pl.semaphore_signal(barrier, inc=1, device_id={"seq": q}, device_id_type=MESH)
    pl.semaphore_wait(barrier, len(peers) + len(mates) + 1)

    def hop(buf, ssem, rsem, side, j, c, g):
        r = pl.ds(c * crow + g * srow, srow)
        to = t + 1 if side == 0 else t - 1
        return pltpu.make_async_remote_copy(
            src_ref=buf.at[j, r],
            dst_ref=buf.at[j, r],
            send_sem=ssem.at[side, j, c * SUBS + g],
            recv_sem=rsem.at[j, c * SUBS + g],
            device_id={"tensor": to},
            device_id_type=MESH,
        )

    def gather_start(buf, ssem, rsem, c):
        for g in range(SUBS):
            @pl.when(t < n - 1)
            def _():
                hop(buf, ssem, rsem, 0, t, c, g).start()

            @pl.when(t > 0)
            def _():
                hop(buf, ssem, rsem, 1, t, c, g).start()

    def gather_pass(buf, ssem, rsem, c, d):
        for g in range(SUBS):
            @pl.when(t - d >= 0)
            def _():
                j = t - d
                hop(buf, ssem, rsem, 0, j, c, g).wait_recv()

                @pl.when(t < n - 1)
                def _():
                    hop(buf, ssem, rsem, 0, j, c, g).start()

            @pl.when(t + d < n)
            def _():
                j = t + d
                hop(buf, ssem, rsem, 1, j, c, g).wait_recv()

                @pl.when(t > 0)
                def _():
                    hop(buf, ssem, rsem, 1, j, c, g).start()

    def gather_drain(buf, ssem, rsem):
        def body(j, carry):
            for c in range(CHUNKS):
                for g in range(SUBS):
                    @pl.when((t < n - 1) & (j <= t))
                    def _():
                        hop(buf, ssem, rsem, 0, j, c, g).wait_send()

                    @pl.when((t > 0) & (j >= t))
                    def _():
                        hop(buf, ssem, rsem, 1, j, c, g).wait_send()
            return carry

        lax.fori_loop(0, n, body, 0)

    def on_blocks(d, work):
        def body(i, carry):
            j = t - d + 2 * d * i

            @pl.when((j >= 0) & (j < n) & ((d > 0) | (i == 0)))
            def _():
                work(j)
            return carry

        lax.fori_loop(0, 2, body, 0)

    def project(c, j):
        if c == 0:
            w_in(0, wg_hbm, wg, j).wait()
            w_in(1, wu_hbm, wu, j).wait()
        x = xs[j, pl.ds(c * crow, crow), :].astype(jnp.float32)
        rsq[...] += jnp.sum(x * x, axis=1, keepdims=True)
        xg = (x * fg_ref[:, fblk(j)]).astype(jnp.bfloat16)
        gate[...] += jnp.dot(xg, wg[fblk(j), :], preferred_element_type=jnp.float32)
        up[...] += jnp.dot(xg, wu[fblk(j), :], preferred_element_type=jnp.float32)

    def enter_in(c):
        gate[...] = jnp.zeros_like(gate)
        up[...] = jnp.zeros_like(up)
        rsq[...] = jnp.zeros_like(rsq)
        x_copy(c).wait()
        gather_start(xs, a1s, a1r, c)

    def in_step(c, d):
        @pl.when(d > 0)
        def _():
            gather_pass(xs, a1s, a1r, c, d)
        on_blocks(d, functools.partial(project, c))

    def make_hidden():
        rstd = lax.rsqrt(rsq[...] / width + epsilon)
        hid[...] = (jax.nn.gelu(gate[...] * rstd, approximate=True) * (up[...] * rstd)).astype(jnp.bfloat16)

    def sum_hop(side, j, c, g):
        r = pl.ds(c * crow + g * srow, srow)
        dst = from_left if side == 0 else from_right
        return pltpu.make_async_remote_copy(
            src_ref=sent.at[j, r],
            dst_ref=dst.at[j, r],
            send_sem=rss.at[j, c * SUBS + g],
            recv_sem=rsr.at[side, j, c * SUBS + g],
            device_id={"tensor": t + 1 if side == 0 else t - 1},
            device_id_type=MESH,
        )

    def product(j):
        part[...] = jnp.dot(hid[...], wo[:, fblk(j)], preferred_element_type=jnp.float32)

    def sum_send(side, j, c):
        arrives = (t > 0) if side == 0 else (t < n - 1)
        buf = from_left if side == 0 else from_right
        for g in range(SUBS):
            r = pl.ds(c * crow + g * srow, srow)
            pr = pl.ds(g * srow, srow)

            @pl.when(arrives)
            def _():
                sum_hop(side, j, c, g).wait_recv()
                sent[j, r, :] = (part[pr, :] + buf[j, r, :].astype(jnp.float32)).astype(jnp.bfloat16)

            @pl.when(jnp.logical_not(arrives))
            def _():
                sent[j, r, :] = part[pr, :].astype(jnp.bfloat16)
            sum_hop(side, j, c, g).start()

    def sum_step(c, d):
        @pl.when(d >= t)
        def _():
            j = n - 1 - (d - t)
            product(j)
            sum_send(0, j, c)

        @pl.when(d >= n - 1 - t)
        def _():
            j = d - (n - 1 - t)
            product(j)
            sum_send(1, j, c)

    def sum_own(c):
        r = pl.ds(c * crow, crow)
        product(t)
        part[...] += xs[t, r, :].astype(jnp.float32)

        @pl.when(t > 0)
        def _():
            for g in range(SUBS):
                sum_hop(0, t, c, g).wait_recv()
            part[...] += from_left[t, r, :].astype(jnp.float32)

        @pl.when(t < n - 1)
        def _():
            for g in range(SUBS):
                sum_hop(1, t, c, g).wait_recv()
            part[...] += from_right[t, r, :].astype(jnp.float32)
        mix = part[...]
        scaled = mix * eg_ref[:, fblk(t)]
        ms[t, r, :] = scaled.astype(jnp.bfloat16)
        mixed[c] = scaled
        gather_start(ms, a2s, a2r, c)
        total = jnp.sum(mix * mix, axis=1, keepdims=True)
        ssq[c, t] = jnp.transpose(jnp.broadcast_to(total, (crow, 128)), (1, 0))[:8]
        for p in peers:
            sq_copy(c, t, p).start()

    def sq_copy(c, j, p):
        return pltpu.make_async_remote_copy(
            src_ref=ssq.at[c, j],
            dst_ref=ssq.at[c, j],
            send_sem=sqs.at[c, p],
            recv_sem=sqr.at[c, j],
            device_id={"tensor": p},
            device_id_type=MESH,
        )

    def key_value(c, j):
        if c == 0:
            w_in(2, wk_hbm, wk, j).wait()
            w_in(3, wv_hbm, wv, j).wait()
        y = ms[j, pl.ds(c * crow, crow), :]
        kacc[...] += jnp.dot(y, wk[fblk(j), :], preferred_element_type=jnp.float32)
        vacc[...] += jnp.dot(y, wv[fblk(j), :], preferred_element_type=jnp.float32)

    def out_step(c, d):
        @pl.when(d > 0)
        def _():
            gather_pass(ms, a2s, a2r, c, d)
        on_blocks(d, functools.partial(key_value, c))

    def enter_out():
        kacc[...] = jnp.zeros_like(kacc)
        vacc[...] = jnp.zeros_like(vacc)

    def kv_copy(c, owner, slot, to):
        return pltpu.make_async_remote_copy(
            src_ref=kv.at[owner, c],
            dst_ref=kv.at[owner, c],
            send_sem=kvs.at[slot, c],
            recv_sem=kvr.at[owner, c],
            device_id={"seq": to},
            device_id_type=MESH,
        )

    def store_kv(c, owner, slot):
        r = pl.ds(pl.multiple_of(owner * rows + c * crow, crow), crow)
        return (
            pltpu.make_async_copy(kv.at[owner, c, 0], key_hbm.at[r], osem.at[0, slot, c]),
            pltpu.make_async_copy(kv.at[owner, c, 1], val_hbm.at[r], osem.at[1, slot, c]),
        )

    def enc_store(c):
        r = pl.ds(c * crow, crow)
        return pltpu.make_async_copy(enc.at[r], enc_hbm.at[r], osem.at[0, m, c])

    def finish(c):
        total = ssq[c, t]
        for p in peers:
            sq_copy(c, p, p).wait_recv()
            total = total + ssq[c, p]
        column = jnp.transpose(jnp.broadcast_to(total[:1], (128, crow)), (1, 0))[:, :1]
        rstd = lax.rsqrt(column / width + epsilon)
        kv[s, c, 0] = (kacc[...] * rstd).astype(jnp.bfloat16)
        kv[s, c, 1] = (vacc[...] * rstd).astype(jnp.bfloat16)
        for i, q in enumerate(mates):
            kv_copy(c, s, i, q).start()
        kv_copy(c, s, m - 1, partner).start()
        enc[pl.ds(c * crow, crow), :] = (mixed[c] * rstd).astype(jnp.bfloat16)
        enc_store(c).start()
        for cp in store_kv(c, s, 0):
            cp.start()

    def pass_kv(c):
        for i, q in enumerate(mates):
            kv_copy(c, q, i, q).wait_recv()
            kv_copy(c, q, len(mates) + i, partner).start()
            for cp in store_kv(c, q, 1 + i):
                cp.start()

    def take_kv(c):
        for i in range(m // 2):
            q = lax.rem(partner + 2 * i, m)
            kv_copy(c, q, m - 1, partner).wait_recv()
            for cp in store_kv(c, q, m // 2 + i):
                cp.start()

    def steps(lo, hi, *works):
        def body(d, carry):
            for w in works:
                w(d)
            return carry

        lax.fori_loop(lo, hi, body, 0)

    def at(f, c):
        return functools.partial(f, c)

    last = n - 1
    enter_in(0)
    steps(0, n, at(in_step, 0))
    make_hidden()
    wo_copy.wait()
    for c in range(CHUNKS):
        more = c + 1 < CHUNKS
        before = c > 0
        if more:
            enter_in(c + 1)
        if before:
            enter_out()
        works = []
        if more:
            works.append(at(in_step, c + 1))
        if before:
            works.append(at(out_step, c - 1))
        steps(0, last, *(works + [at(sum_step, c)]))
        for w in works:
            w(jnp.int32(last))
        sum_own(c)
        if before:
            finish(c - 1)
        if more:
            make_hidden()
    c = CHUNKS - 1
    enter_out()
    steps(0, n, at(out_step, c))
    finish(c)
    for b in range(CHUNKS):
        pass_kv(b)
    for b in range(CHUNKS):
        take_kv(b)

    gather_drain(xs, a1s, a1r)
    gather_drain(ms, a2s, a2r)

    def sums_drain(j, carry):
        for c in range(CHUNKS):
            for g in range(SUBS):
                @pl.when(j > t)
                def _():
                    sum_hop(0, j, c, g).wait_send()

                @pl.when(j < t)
                def _():
                    sum_hop(1, j, c, g).wait_send()
        return carry

    lax.fori_loop(0, n, sums_drain, 0)
    for c in range(CHUNKS):
        for p in peers:
            sq_copy(c, t, p).wait_send()
        for i, q in enumerate(mates):
            kv_copy(c, s, i, q).wait_send()
            kv_copy(c, q, len(mates) + i, partner).wait_send()
        kv_copy(c, s, m - 1, partner).wait_send()
        enc_store(c).wait()
        for slot in range(m):
            for cp in store_kv(c, s, slot):
                cp.wait()


def on_device(n, m, stream, ffn_gain, final_gain, w_gate, w_up, w_out, w_key, w_value):
    rows, feat = stream.shape
    width = n * feat
    ffc = w_gate.shape[1]
    kvc = w_key.shape[1]
    crow = rows // CHUNKS
    bf, f32 = jnp.bfloat16, jnp.float32
    dma = pltpu.SemaphoreType.DMA
    any_spec = pl.BlockSpec(memory_space=pl.ANY)
    vmem = pl.BlockSpec(memory_space=pltpu.VMEM)
    parts = CHUNKS * SUBS
    return pl.pallas_call(
        functools.partial(block_kernel, n, m),
        out_shape=(
            jax.ShapeDtypeStruct((rows, feat), bf),
            jax.ShapeDtypeStruct((m * rows, kvc), bf),
            jax.ShapeDtypeStruct((m * rows, kvc), bf),
        ),
        in_specs=[any_spec, vmem, vmem] + [any_spec] * 5,
        out_specs=(any_spec,) * 3,
        scratch_shapes=[
            pltpu.VMEM((width, ffc), bf),
            pltpu.VMEM((width, ffc), bf),
            pltpu.VMEM((ffc, width), bf),
            pltpu.VMEM((width, kvc), bf),
            pltpu.VMEM((width, kvc), bf),
            pltpu.VMEM((n, rows, feat), bf),
            pltpu.VMEM((n, rows, feat), bf),
            pltpu.VMEM((n, rows, feat), bf),
            pltpu.VMEM((n, rows, feat), bf),
            pltpu.VMEM((n, rows, feat), bf),
            pltpu.VMEM((crow, ffc), f32),
            pltpu.VMEM((crow, ffc), f32),
            pltpu.VMEM((crow, ffc), bf),
            pltpu.VMEM((crow, feat), f32),
            pltpu.VMEM((CHUNKS, crow, feat), f32),
            pltpu.VMEM((CHUNKS, n, 8, crow), f32),
            pltpu.VMEM((crow, kvc), f32),
            pltpu.VMEM((crow, kvc), f32),
            pltpu.VMEM((crow, 1), f32),
            pltpu.VMEM((rows, feat), bf),
            pltpu.VMEM((m, CHUNKS, 2, crow, kvc), bf),
            dma((5, n)),
            dma((CHUNKS,)),
            dma((2, n, parts)),
            dma((n, parts)),
            dma((n, parts)),
            dma((2, n, parts)),
            dma((2, n, parts)),
            dma((n, parts)),
            dma((CHUNKS, n)),
            dma((CHUNKS, n)),
            dma((m, CHUNKS)),
            dma((m, CHUNKS)),
            dma((2, m + 1, CHUNKS)),
        ],
        compiler_params=pltpu.CompilerParams(
            collective_id=0, has_side_effects=True, vmem_limit_bytes=67000000
        ),
    )(
        stream,
        ffn_gain.reshape(1, width),
        final_gain.reshape(1, width),
        w_gate, w_up, w_out, w_key, w_value,
    )


def solution(mesh):
    placed = (
        P(("groups", "seq"), "tensor"),
        P(),
        P(),
        P(None, "tensor"),
        P(None, "tensor"),
        P("tensor", None),
        P(None, "tensor"),
        P(None, "tensor"),
    )
    return jax.shard_map(
        functools.partial(on_device, mesh.shape["tensor"], mesh.shape["seq"]),
        mesh=mesh,
        in_specs=placed,
        out_specs=(P(("groups", "seq"), "tensor"), P("groups", "tensor"), P("groups", "tensor")),
        check_vma=False,
    )
```

```python
import functools

import jax
import jax.numpy as jnp
from jax import lax
from jax.experimental import pallas as pl
from jax.experimental.pallas import tpu as pltpu
from jax.sharding import PartitionSpec as P

epsilon = 1e-06
MESH = pl.DeviceIdType.MESH
CHUNKS = 2
SUBS = 2


def block_kernel(
    n, m,
    x_hbm, fg_ref, eg_ref, wg_hbm, wu_hbm, wo_hbm, wk_hbm, wv_hbm,
    enc_hbm, key_hbm, val_hbm,
    wg, wu, wo, wk, wv,
    xs, ms, sent, from_left, from_right,
    gate, up, hid, part, mixed, ssq, kacc, vacc, rsq, enc, kv,
    wsem, xsem, a1s, a1r, rss, rsr, a2s, a2r, sqs, sqr, kvs, kvr, osem,
):
    t = lax.axis_index("tensor")
    s = lax.axis_index("seq")
    _, rows, feat = xs.shape
    crow = rows // CHUNKS
    srow = crow // SUBS
    width = n * feat
    partner = s + 1 - 2 * lax.rem(s, 2)
    mates = [lax.rem(s + 2 * d, m) for d in range(1, m // 2)]
    peers = [lax.rem(t + d, n) for d in range(1, n)]

    def fblk(j):
        return pl.ds(pl.multiple_of(j * feat, feat), feat)

    def x_copy(c):
        r = pl.ds(c * crow, crow)
        return pltpu.make_async_copy(x_hbm.at[r], xs.at[t, r], xsem.at[c])

    def w_in(i, src, dst, j):
        return pltpu.make_async_copy(src.at[fblk(j)], dst.at[fblk(j)], wsem.at[i, j])

    wo_copy = pltpu.make_async_copy(wo_hbm, wo, wsem.at[4, 0])
    for c in range(CHUNKS):
        x_copy(c).start()

    def first_weights(d, carry):
        j = lax.rem(t + d, n)
        w_in(0, wg_hbm, wg, j).start()
        w_in(1, wu_hbm, wu, j).start()
        return carry

    def last_weights(d, carry):
        w_in(2, wk_hbm, wk, d).start()
        w_in(3, wv_hbm, wv, d).start()
        return carry

    lax.fori_loop(0, n, first_weights, 0)
    wo_copy.start()
    lax.fori_loop(0, n, last_weights, 0)

    barrier = pltpu.get_barrier_semaphore()
    for p in peers:
        pl.semaphore_signal(barrier, inc=1, device_id={"tensor": p}, device_id_type=MESH)
    for q in mates + [partner]:
        pl.semaphore_signal(barrier, inc=1, device_id={"seq": q}, device_id_type=MESH)
    pl.semaphore_wait(barrier, len(peers) + len(mates) + 1)

    def hop(buf, ssem, rsem, side, j, c, g):
        r = pl.ds(c * crow + g * srow, srow)
        to = t + 1 if side == 0 else t - 1
        return pltpu.make_async_remote_copy(
            src_ref=buf.at[j, r],
            dst_ref=buf.at[j, r],
            send_sem=ssem.at[side, j, c * SUBS + g],
            recv_sem=rsem.at[j, c * SUBS + g],
            device_id={"tensor": to},
            device_id_type=MESH,
        )

    def gather_start(buf, ssem, rsem, c, up_too=True, down_too=True):
        for g in range(SUBS):
            @pl.when((t < n - 1) & up_too)
            def _():
                hop(buf, ssem, rsem, 0, t, c, g).start()

            @pl.when((t > 0) & down_too)
            def _():
                hop(buf, ssem, rsem, 1, t, c, g).start()

    def gather_pass(buf, ssem, rsem, c, d):
        for g in range(SUBS):
            @pl.when(t - d >= 0)
            def _():
                j = t - d
                hop(buf, ssem, rsem, 0, j, c, g).wait_recv()

                @pl.when(t < n - 1)
                def _():
                    hop(buf, ssem, rsem, 0, j, c, g).start()

            @pl.when(t + d < n)
            def _():
                j = t + d
                hop(buf, ssem, rsem, 1, j, c, g).wait_recv()

                @pl.when(t > 0)
                def _():
                    hop(buf, ssem, rsem, 1, j, c, g).start()

    def gather_drain(buf, ssem, rsem):
        def body(j, carry):
            for c in range(CHUNKS):
                for g in range(SUBS):
                    @pl.when((t < n - 1) & (j <= t))
                    def _():
                        hop(buf, ssem, rsem, 0, j, c, g).wait_send()

                    @pl.when((t > 0) & (j >= t))
                    def _():
                        hop(buf, ssem, rsem, 1, j, c, g).wait_send()
            return carry

        lax.fori_loop(0, n, body, 0)

    def on_blocks(d, work):
        def body(i, carry):
            j = t - d + 2 * d * i

            @pl.when((j >= 0) & (j < n) & ((d > 0) | (i == 0)))
            def _():
                work(j)
            return carry

        lax.fori_loop(0, 2, body, 0)

    def project(c, j):
        if c == 0:
            w_in(0, wg_hbm, wg, j).wait()
            w_in(1, wu_hbm, wu, j).wait()
        x = xs[j, pl.ds(c * crow, crow), :].astype(jnp.float32)
        rsq[...] += jnp.sum(x * x, axis=1, keepdims=True)
        xg = (x * fg_ref[:, fblk(j)]).astype(jnp.bfloat16)
        gate[...] += jnp.dot(xg, wg[fblk(j), :], preferred_element_type=jnp.float32)
        up[...] += jnp.dot(xg, wu[fblk(j), :], preferred_element_type=jnp.float32)

    def enter_in(c):
        gate[...] = jnp.zeros_like(gate)
        up[...] = jnp.zeros_like(up)
        rsq[...] = jnp.zeros_like(rsq)

    def in_step(c, d):
        @pl.when(d > 0)
        def _():
            gather_pass(xs, a1s, a1r, c, d)
        if c + 1 < CHUNKS:
            gather_start(xs, a1s, a1r, c + 1, d == t, d == n - 1 - t)
        on_blocks(d, functools.partial(project, c))

    def make_hidden():
        rstd = lax.rsqrt(rsq[...] / width + epsilon)
        hid[...] = (jax.nn.gelu(gate[...] * rstd, approximate=True) * (up[...] * rstd)).astype(jnp.bfloat16)

    def sum_hop(side, j, c, g):
        r = pl.ds(c * crow + g * srow, srow)
        dst = from_left if side == 0 else from_right
        return pltpu.make_async_remote_copy(
            src_ref=sent.at[j, r],
            dst_ref=dst.at[j, r],
            send_sem=rss.at[j, c * SUBS + g],
            recv_sem=rsr.at[side, j, c * SUBS + g],
            device_id={"tensor": t + 1 if side == 0 else t - 1},
            device_id_type=MESH,
        )

    def product(j):
        part[...] = jnp.dot(hid[...], wo[:, fblk(j)], preferred_element_type=jnp.float32)

    def sum_send(side, j, c):
        arrives = (t > 0) if side == 0 else (t < n - 1)
        buf = from_left if side == 0 else from_right
        for g in range(SUBS):
            r = pl.ds(c * crow + g * srow, srow)
            pr = pl.ds(g * srow, srow)

            @pl.when(arrives)
            def _():
                sum_hop(side, j, c, g).wait_recv()
                sent[j, r, :] = (part[pr, :] + buf[j, r, :].astype(jnp.float32)).astype(jnp.bfloat16)

            @pl.when(jnp.logical_not(arrives))
            def _():
                sent[j, r, :] = part[pr, :].astype(jnp.bfloat16)
            sum_hop(side, j, c, g).start()

    def sum_step(c, d):
        @pl.when(d >= t)
        def _():
            j = n - 1 - (d - t)
            product(j)
            sum_send(0, j, c)

        @pl.when(d >= n - 1 - t)
        def _():
            j = d - (n - 1 - t)
            product(j)
            sum_send(1, j, c)

    def sum_own(c):
        r = pl.ds(c * crow, crow)
        product(t)
        part[...] += xs[t, r, :].astype(jnp.float32)

        @pl.when(t > 0)
        def _():
            for g in range(SUBS):
                sum_hop(0, t, c, g).wait_recv()
            part[...] += from_left[t, r, :].astype(jnp.float32)

        @pl.when(t < n - 1)
        def _():
            for g in range(SUBS):
                sum_hop(1, t, c, g).wait_recv()
            part[...] += from_right[t, r, :].astype(jnp.float32)
        mix = part[...]
        scaled = mix * eg_ref[:, fblk(t)]
        ms[t, r, :] = scaled.astype(jnp.bfloat16)
        mixed[c] = scaled
        gather_start(ms, a2s, a2r, c)
        total = jnp.sum(mix * mix, axis=1, keepdims=True)
        ssq[c, t] = jnp.transpose(jnp.broadcast_to(total, (crow, 128)), (1, 0))[:8]
        for p in peers:
            sq_copy(c, t, p).start()

    def sq_copy(c, j, p):
        return pltpu.make_async_remote_copy(
            src_ref=ssq.at[c, j],
            dst_ref=ssq.at[c, j],
            send_sem=sqs.at[c, p],
            recv_sem=sqr.at[c, j],
            device_id={"tensor": p},
            device_id_type=MESH,
        )

    def key_value(c, j):
        if c == 0:
            w_in(2, wk_hbm, wk, j).wait()
            w_in(3, wv_hbm, wv, j).wait()
        y = ms[j, pl.ds(c * crow, crow), :]
        kacc[...] += jnp.dot(y, wk[fblk(j), :], preferred_element_type=jnp.float32)
        vacc[...] += jnp.dot(y, wv[fblk(j), :], preferred_element_type=jnp.float32)

    def out_step(c, d):
        @pl.when(d > 0)
        def _():
            gather_pass(ms, a2s, a2r, c, d)
        on_blocks(d, functools.partial(key_value, c))

    def enter_out():
        kacc[...] = jnp.zeros_like(kacc)
        vacc[...] = jnp.zeros_like(vacc)

    def kv_copy(c, owner, slot, to):
        return pltpu.make_async_remote_copy(
            src_ref=kv.at[owner, c],
            dst_ref=kv.at[owner, c],
            send_sem=kvs.at[slot, c],
            recv_sem=kvr.at[owner, c],
            device_id={"seq": to},
            device_id_type=MESH,
        )

    def store_kv(c, owner, slot):
        r = pl.ds(pl.multiple_of(owner * rows + c * crow, crow), crow)
        return (
            pltpu.make_async_copy(kv.at[owner, c, 0], key_hbm.at[r], osem.at[0, slot, c]),
            pltpu.make_async_copy(kv.at[owner, c, 1], val_hbm.at[r], osem.at[1, slot, c]),
        )

    def enc_store(c):
        r = pl.ds(c * crow, crow)
        return pltpu.make_async_copy(enc.at[r], enc_hbm.at[r], osem.at[0, m, c])

    def finish(c):
        total = ssq[c, t]
        for p in peers:
            sq_copy(c, p, p).wait_recv()
            total = total + ssq[c, p]
        column = jnp.transpose(jnp.broadcast_to(total[:1], (128, crow)), (1, 0))[:, :1]
        rstd = lax.rsqrt(column / width + epsilon)
        kv[s, c, 0] = (kacc[...] * rstd).astype(jnp.bfloat16)
        kv[s, c, 1] = (vacc[...] * rstd).astype(jnp.bfloat16)
        for i, q in enumerate(mates):
            kv_copy(c, s, i, q).start()
        kv_copy(c, s, m - 1, partner).start()
        enc[pl.ds(c * crow, crow), :] = (mixed[c] * rstd).astype(jnp.bfloat16)
        enc_store(c).start()
        for cp in store_kv(c, s, 0):
            cp.start()

    def pass_kv(c):
        for i, q in enumerate(mates):
            kv_copy(c, q, i, q).wait_recv()
            kv_copy(c, q, len(mates) + i, partner).start()
            for cp in store_kv(c, q, 1 + i):
                cp.start()

    def take_kv(c):
        for i in range(m // 2):
            q = lax.rem(partner + 2 * i, m)
            kv_copy(c, q, m - 1, partner).wait_recv()
            for cp in store_kv(c, q, m // 2 + i):
                cp.start()

    def steps(lo, hi, *works):
        def body(d, carry):
            for w in works:
                w(d)
            return carry

        lax.fori_loop(lo, hi, body, 0)

    def at(f, c):
        return functools.partial(f, c)

    last = n - 1
    for c in range(CHUNKS):
        x_copy(c).wait()
    gather_start(xs, a1s, a1r, 0)
    enter_in(0)
    steps(0, n, at(in_step, 0))
    make_hidden()
    wo_copy.wait()
    for c in range(CHUNKS):
        more = c + 1 < CHUNKS
        before = c > 0
        if more:
            enter_in(c + 1)
        if before:
            enter_out()
        works = []
        if more:
            works.append(at(in_step, c + 1))
        if before:
            works.append(at(out_step, c - 1))
        steps(0, last, *(works + [at(sum_step, c)]))
        for w in works:
            w(jnp.int32(last))
        sum_own(c)
        if before:
            finish(c - 1)
        if more:
            make_hidden()
    c = CHUNKS - 1
    enter_out()
    steps(0, n, at(out_step, c))
    finish(c)
    for b in range(CHUNKS):
        pass_kv(b)
    for b in range(CHUNKS):
        take_kv(b)

    gather_drain(xs, a1s, a1r)
    gather_drain(ms, a2s, a2r)

    def sums_drain(j, carry):
        for c in range(CHUNKS):
            for g in range(SUBS):
                @pl.when(j > t)
                def _():
                    sum_hop(0, j, c, g).wait_send()

                @pl.when(j < t)
                def _():
                    sum_hop(1, j, c, g).wait_send()
        return carry

    lax.fori_loop(0, n, sums_drain, 0)
    for c in range(CHUNKS):
        for p in peers:
            sq_copy(c, t, p).wait_send()
        for i, q in enumerate(mates):
            kv_copy(c, s, i, q).wait_send()
            kv_copy(c, q, len(mates) + i, partner).wait_send()
        kv_copy(c, s, m - 1, partner).wait_send()
        enc_store(c).wait()
        for slot in range(m):
            for cp in store_kv(c, s, slot):
                cp.wait()


def write_kernel(pieces, *refs):
    count = (len(refs) - 2) // 3
    srcs, dsts, bufs = refs[:count], refs[count:2 * count], refs[2 * count:3 * count]
    isem, wsem = refs[3 * count:]
    loads, stores = [], []
    for i in range(count):
        size = srcs[i].shape[0] // pieces
        for k in range(pieces):
            r = pl.ds(k * size, size)
            loads.append(pltpu.make_async_copy(srcs[i].at[r], bufs[i].at[r], isem.at[i, k]))
            stores.append(pltpu.make_async_copy(bufs[i].at[r], dsts[i].at[r], wsem.at[i, k]))
    for load in loads:
        load.start()
    for load, store in zip(loads, stores):
        load.wait()
        store.start()
    for store in stores:
        store.wait()


def write_out(arrays):
    count, pieces = len(arrays), 2
    any_spec = pl.BlockSpec(memory_space=pl.ANY)
    return pl.pallas_call(
        functools.partial(write_kernel, pieces),
        out_shape=tuple(jax.ShapeDtypeStruct(a.shape, a.dtype) for a in arrays),
        in_specs=[any_spec] * count,
        out_specs=(any_spec,) * count,
        scratch_shapes=[pltpu.VMEM(a.shape, a.dtype) for a in arrays]
        + [pltpu.SemaphoreType.DMA((count, pieces))] * 2,
    )(*arrays)


def on_device(n, m, stream, ffn_gain, final_gain, w_gate, w_up, w_out, w_key, w_value):
    rows, feat = stream.shape
    width = n * feat
    ffc = w_gate.shape[1]
    kvc = w_key.shape[1]
    crow = rows // CHUNKS
    bf, f32 = jnp.bfloat16, jnp.float32
    dma = pltpu.SemaphoreType.DMA
    any_spec = pl.BlockSpec(memory_space=pl.ANY)
    vmem = pl.BlockSpec(memory_space=pltpu.VMEM)
    parts = CHUNKS * SUBS
    made = pl.pallas_call(
        functools.partial(block_kernel, n, m),
        out_shape=(
            jax.ShapeDtypeStruct((rows, feat), bf),
            jax.ShapeDtypeStruct((m * rows, kvc), bf),
            jax.ShapeDtypeStruct((m * rows, kvc), bf),
        ),
        in_specs=[any_spec, vmem, vmem] + [any_spec] * 5,
        out_specs=(any_spec,) * 3,
        scratch_shapes=[
            pltpu.VMEM((width, ffc), bf),
            pltpu.VMEM((width, ffc), bf),
            pltpu.VMEM((ffc, width), bf),
            pltpu.VMEM((width, kvc), bf),
            pltpu.VMEM((width, kvc), bf),
            pltpu.VMEM((n, rows, feat), bf),
            pltpu.VMEM((n, rows, feat), bf),
            pltpu.VMEM((n, rows, feat), bf),
            pltpu.VMEM((n, rows, feat), bf),
            pltpu.VMEM((n, rows, feat), bf),
            pltpu.VMEM((crow, ffc), f32),
            pltpu.VMEM((crow, ffc), f32),
            pltpu.VMEM((crow, ffc), bf),
            pltpu.VMEM((crow, feat), f32),
            pltpu.VMEM((CHUNKS, crow, feat), f32),
            pltpu.VMEM((CHUNKS, n, 8, crow), f32),
            pltpu.VMEM((crow, kvc), f32),
            pltpu.VMEM((crow, kvc), f32),
            pltpu.VMEM((crow, 1), f32),
            pltpu.VMEM((rows, feat), bf),
            pltpu.VMEM((m, CHUNKS, 2, crow, kvc), bf),
            dma((5, n)),
            dma((CHUNKS,)),
            dma((2, n, parts)),
            dma((n, parts)),
            dma((n, parts)),
            dma((2, n, parts)),
            dma((2, n, parts)),
            dma((n, parts)),
            dma((CHUNKS, n)),
            dma((CHUNKS, n)),
            dma((m, CHUNKS)),
            dma((m, CHUNKS)),
            dma((2, m + 1, CHUNKS)),
        ],
        compiler_params=pltpu.CompilerParams(
            collective_id=0, has_side_effects=True, vmem_limit_bytes=67000000
        ),
    )(
        stream,
        ffn_gain.reshape(1, width),
        final_gain.reshape(1, width),
        w_gate, w_up, w_out, w_key, w_value,
    )
    return write_out(made)


def solution(mesh):
    placed = (
        P(("groups", "seq"), "tensor"),
        P(),
        P(),
        P(None, "tensor"),
        P(None, "tensor"),
        P("tensor", None),
        P(None, "tensor"),
        P(None, "tensor"),
    )
    return jax.shard_map(
        functools.partial(on_device, mesh.shape["tensor"], mesh.shape["seq"]),
        mesh=mesh,
        in_specs=placed,
        out_specs=(P(("groups", "seq"), "tensor"), P("groups", "tensor"), P("groups", "tensor")),
        check_vma=False,
    )
```

```python
import functools

import jax
import jax.numpy as jnp
from jax import lax
from jax.experimental import pallas as pl
from jax.experimental.pallas import tpu as pltpu
from jax.sharding import PartitionSpec as P

epsilon = 1e-06
MESH = pl.DeviceIdType.MESH
CHUNKS = 2
SUBS = 2


def block_kernel(
    n, m,
    x_hbm, fg_ref, eg_ref, wg_hbm, wu_hbm, wo_hbm, wk_hbm, wv_hbm,
    enc_hbm, key_hbm, val_hbm,
    wg, wu, wo, wk, wv,
    xs, ms, sent, from_left, from_right,
    gate, up, hid, part, mixed, ssq, kacc, vacc, rsq, rsq2, enc, kv,
    wsem, xsem, a1s, a1r, rss, rsr, a2s, a2r, sqs, sqr, kvs, kvr, osem,
):
    t = lax.axis_index("tensor")
    s = lax.axis_index("seq")
    _, rows, feat = xs.shape
    crow = rows // CHUNKS
    srow = crow // SUBS
    width = n * feat
    partner = s + 1 - 2 * lax.rem(s, 2)
    mates = [lax.rem(s + 2 * d, m) for d in range(1, m // 2)]
    peers = [lax.rem(t + d, n) for d in range(1, n)]

    def fblk(j):
        return pl.ds(pl.multiple_of(j * feat, feat), feat)

    def x_copy(c):
        r = pl.ds(c * crow, crow)
        return pltpu.make_async_copy(x_hbm.at[r], xs.at[t, r], xsem.at[c])

    def w_in(i, src, dst, j):
        return pltpu.make_async_copy(src.at[fblk(j)], dst.at[fblk(j)], wsem.at[i, j])

    wo_copy = pltpu.make_async_copy(wo_hbm, wo, wsem.at[4, 0])
    for c in range(CHUNKS):
        x_copy(c).start()

    def first_weights(d, carry):
        j = lax.rem(t + d, n)
        w_in(0, wg_hbm, wg, j).start()
        w_in(1, wu_hbm, wu, j).start()
        return carry

    def last_weights(d, carry):
        w_in(2, wk_hbm, wk, d).start()
        w_in(3, wv_hbm, wv, d).start()
        return carry

    lax.fori_loop(0, n, first_weights, 0)
    wo_copy.start()
    lax.fori_loop(0, n, last_weights, 0)

    barrier = pltpu.get_barrier_semaphore()
    for p in peers:
        pl.semaphore_signal(barrier, inc=1, device_id={"tensor": p}, device_id_type=MESH)
    for q in mates + [partner]:
        pl.semaphore_signal(barrier, inc=1, device_id={"seq": q}, device_id_type=MESH)
    pl.semaphore_wait(barrier, len(peers) + len(mates) + 1)

    def hop(buf, ssem, rsem, side, j, c, g):
        r = pl.ds(c * crow + g * srow, srow)
        to = t + 1 if side == 0 else t - 1
        return pltpu.make_async_remote_copy(
            src_ref=buf.at[j, r],
            dst_ref=buf.at[j, r],
            send_sem=ssem.at[side, j, c * SUBS + g],
            recv_sem=rsem.at[j, c * SUBS + g],
            device_id={"tensor": to},
            device_id_type=MESH,
        )

    def gather_start(buf, ssem, rsem, c, up_too=True, down_too=True):
        for g in range(SUBS):
            @pl.when((t < n - 1) & up_too)
            def _():
                hop(buf, ssem, rsem, 0, t, c, g).start()

            @pl.when((t > 0) & down_too)
            def _():
                hop(buf, ssem, rsem, 1, t, c, g).start()

    def gather_pass(buf, ssem, rsem, c, d, subs=range(SUBS)):
        for g in subs:
            @pl.when(t - d >= 0)
            def _():
                j = t - d
                hop(buf, ssem, rsem, 0, j, c, g).wait_recv()

                @pl.when(t < n - 1)
                def _():
                    hop(buf, ssem, rsem, 0, j, c, g).start()

            @pl.when(t + d < n)
            def _():
                j = t + d
                hop(buf, ssem, rsem, 1, j, c, g).wait_recv()

                @pl.when(t > 0)
                def _():
                    hop(buf, ssem, rsem, 1, j, c, g).start()

    def gather_drain(buf, ssem, rsem):
        def body(j, carry):
            for c in range(CHUNKS):
                for g in range(SUBS):
                    @pl.when((t < n - 1) & (j <= t))
                    def _():
                        hop(buf, ssem, rsem, 0, j, c, g).wait_send()

                    @pl.when((t > 0) & (j >= t))
                    def _():
                        hop(buf, ssem, rsem, 1, j, c, g).wait_send()
            return carry

        lax.fori_loop(0, n, body, 0)

    def on_blocks(d, work):
        def body(i, carry):
            j = t - d + 2 * d * i

            @pl.when((j >= 0) & (j < n) & ((d > 0) | (i == 0)))
            def _():
                work(j)
            return carry

        lax.fori_loop(0, 2, body, 0)

    def project(c, j):
        if c == 0:
            w_in(0, wg_hbm, wg, j).wait()
            w_in(1, wu_hbm, wu, j).wait()
        x = xs[j, pl.ds(c * crow, crow), :].astype(jnp.float32)
        rsq[...] += jnp.sum(x * x, axis=1, keepdims=True)
        xg = (x * fg_ref[:, fblk(j)]).astype(jnp.bfloat16)
        gate[...] += jnp.dot(xg, wg[fblk(j), :], preferred_element_type=jnp.float32)
        up[...] += jnp.dot(xg, wu[fblk(j), :], preferred_element_type=jnp.float32)

    def enter_in(c):
        gate[...] = jnp.zeros_like(gate)
        up[...] = jnp.zeros_like(up)
        rsq[...] = jnp.zeros_like(rsq)

    def in_step(c, d):
        @pl.when(d > 0)
        def _():
            gather_pass(xs, a1s, a1r, c, d)
        if c + 1 < CHUNKS:
            gather_start(xs, a1s, a1r, c + 1, d == t, d == n - 1 - t)
        on_blocks(d, functools.partial(project, c))

    def make_hidden():
        rstd = lax.rsqrt(rsq[...] / width + epsilon)
        hid[...] = (jax.nn.gelu(gate[...] * rstd, approximate=True) * (up[...] * rstd)).astype(jnp.bfloat16)

    def sum_hop(side, j, c, g):
        r = pl.ds(c * crow + g * srow, srow)
        dst = from_left if side == 0 else from_right
        return pltpu.make_async_remote_copy(
            src_ref=sent.at[j, r],
            dst_ref=dst.at[j, r],
            send_sem=rss.at[j, c * SUBS + g],
            recv_sem=rsr.at[side, j, c * SUBS + g],
            device_id={"tensor": t + 1 if side == 0 else t - 1},
            device_id_type=MESH,
        )

    def product(j):
        part[...] = jnp.dot(hid[...], wo[:, fblk(j)], preferred_element_type=jnp.float32)

    def sum_send(side, j, c):
        arrives = (t > 0) if side == 0 else (t < n - 1)
        buf = from_left if side == 0 else from_right
        for g in range(SUBS):
            r = pl.ds(c * crow + g * srow, srow)
            pr = pl.ds(g * srow, srow)

            @pl.when(arrives)
            def _():
                sum_hop(side, j, c, g).wait_recv()
                sent[j, r, :] = (part[pr, :] + buf[j, r, :].astype(jnp.float32)).astype(jnp.bfloat16)

            @pl.when(jnp.logical_not(arrives))
            def _():
                sent[j, r, :] = part[pr, :].astype(jnp.bfloat16)
            sum_hop(side, j, c, g).start()

    def sum_step(c, d):
        @pl.when(d >= t)
        def _():
            j = n - 1 - (d - t)
            product(j)
            sum_send(0, j, c)

        @pl.when(d >= n - 1 - t)
        def _():
            j = d - (n - 1 - t)
            product(j)
            sum_send(1, j, c)

    def sum_own(c):
        r = pl.ds(c * crow, crow)
        product(t)
        part[...] += xs[t, r, :].astype(jnp.float32)

        @pl.when(t > 0)
        def _():
            for g in range(SUBS):
                sum_hop(0, t, c, g).wait_recv()
            part[...] += from_left[t, r, :].astype(jnp.float32)

        @pl.when(t < n - 1)
        def _():
            for g in range(SUBS):
                sum_hop(1, t, c, g).wait_recv()
            part[...] += from_right[t, r, :].astype(jnp.float32)
        mix = part[...]
        scaled = mix * eg_ref[:, fblk(t)]
        ms[t, r, :] = scaled.astype(jnp.bfloat16)
        mixed[c] = scaled
        gather_start(ms, a2s, a2r, c)
        total = jnp.sum(mix * mix, axis=1, keepdims=True)
        ssq[c, t] = jnp.transpose(jnp.broadcast_to(total, (crow, 128)), (1, 0))[:8]
        for p in peers:
            sq_copy(c, t, p).start()

    def sq_copy(c, j, p):
        return pltpu.make_async_remote_copy(
            src_ref=ssq.at[c, j],
            dst_ref=ssq.at[c, j],
            send_sem=sqs.at[c, p],
            recv_sem=sqr.at[c, j],
            device_id={"tensor": p},
            device_id_type=MESH,
        )

    def key_value(c, j):
        if c == 0:
            w_in(2, wk_hbm, wk, j).wait()
            w_in(3, wv_hbm, wv, j).wait()
        key_value_rows(c, 0, crow, j)

    def key_value_rows(c, at_row, count, j):
        y = ms[j, pl.ds(c * crow + at_row, count), :]
        pr = pl.ds(at_row, count)
        kacc[pr, :] += jnp.dot(y, wk[fblk(j), :], preferred_element_type=jnp.float32)
        vacc[pr, :] += jnp.dot(y, wv[fblk(j), :], preferred_element_type=jnp.float32)

    def out_step(c, d):
        @pl.when(d > 0)
        def _():
            gather_pass(ms, a2s, a2r, c, d)
        on_blocks(d, functools.partial(key_value, c))

    def enter_out():
        kacc[...] = jnp.zeros_like(kacc)
        vacc[...] = jnp.zeros_like(vacc)

    def kv_copy(k, owner, slot, to):
        return pltpu.make_async_remote_copy(
            src_ref=kv.at[owner, k],
            dst_ref=kv.at[owner, k],
            send_sem=kvs.at[slot, k],
            recv_sem=kvr.at[owner, k],
            device_id={"seq": to},
            device_id_type=MESH,
        )

    def store_kv(k, owner, slot):
        r = pl.ds(pl.multiple_of(owner * rows + k * srow, srow), srow)
        return (
            pltpu.make_async_copy(kv.at[owner, k, 0], key_hbm.at[r], osem.at[0, slot, k]),
            pltpu.make_async_copy(kv.at[owner, k, 1], val_hbm.at[r], osem.at[1, slot, k]),
        )

    def enc_store(k):
        r = pl.ds(k * srow, srow)
        return pltpu.make_async_copy(enc.at[r], enc_hbm.at[r], osem.at[0, m, k])

    def final_scale(c):
        total = ssq[c, t]
        for p in peers:
            sq_copy(c, p, p).wait_recv()
            total = total + ssq[c, p]
        column = jnp.transpose(jnp.broadcast_to(total[:1], (128, crow)), (1, 0))[:, :1]
        rsq2[...] = lax.rsqrt(column / width + epsilon)

    def finish(c, g):
        k = c * SUBS + g
        pr = pl.ds(g * srow, srow)
        rstd = rsq2[pr, :]
        kv[s, k, 0] = (kacc[pr, :] * rstd).astype(jnp.bfloat16)
        kv[s, k, 1] = (vacc[pr, :] * rstd).astype(jnp.bfloat16)
        for i, q in enumerate(mates):
            kv_copy(k, s, i, q).start()
        kv_copy(k, s, m - 1, partner).start()
        enc[pl.ds(k * srow, srow), :] = (mixed[c, pr] * rstd).astype(jnp.bfloat16)
        enc_store(k).start()
        for cp in store_kv(k, s, 0):
            cp.start()

    def pass_kv(k):
        for i, q in enumerate(mates):
            kv_copy(k, q, i, q).wait_recv()
            kv_copy(k, q, len(mates) + i, partner).start()
            for cp in store_kv(k, q, 1 + i):
                cp.start()

    def take_kv(k):
        for i in range(m // 2):
            q = lax.rem(partner + 2 * i, m)
            kv_copy(k, q, m - 1, partner).wait_recv()
            for cp in store_kv(k, q, m // 2 + i):
                cp.start()

    def steps(lo, hi, *works):
        def body(d, carry):
            for w in works:
                w(d)
            return carry

        lax.fori_loop(lo, hi, body, 0)

    def at(f, c):
        return functools.partial(f, c)

    last = n - 1
    for c in range(CHUNKS):
        x_copy(c).wait()
    gather_start(xs, a1s, a1r, 0)
    enter_in(0)
    steps(0, n, at(in_step, 0))
    make_hidden()
    wo_copy.wait()
    for c in range(CHUNKS):
        more = c + 1 < CHUNKS
        before = c > 0
        if more:
            enter_in(c + 1)
        if before:
            enter_out()
        works = []
        if more:
            works.append(at(in_step, c + 1))
        if before:
            works.append(at(out_step, c - 1))
        steps(0, last, *(works + [at(sum_step, c)]))
        for w in works:
            w(jnp.int32(last))
        sum_own(c)
        if before:
            final_scale(c - 1)
            for g in range(SUBS):
                finish(c - 1, g)
        if more:
            make_hidden()
    c = CHUNKS - 1
    enter_out()
    steps(0, last, at(out_step, c))
    early = range((CHUNKS - 1) * SUBS)
    late = range((CHUNKS - 1) * SUBS, CHUNKS * SUBS)
    for k in early:
        pass_kv(k)
    final_scale(c)
    for g in range(SUBS):
        gather_pass(ms, a2s, a2r, c, last, (g,))
        on_blocks(jnp.int32(last), functools.partial(key_value_rows, c, g * srow, srow))
        finish(c, g)
    for k in early:
        take_kv(k)
    for k in late:
        pass_kv(k)
    for k in late:
        take_kv(k)

    gather_drain(xs, a1s, a1r)
    gather_drain(ms, a2s, a2r)

    def sums_drain(j, carry):
        for c in range(CHUNKS):
            for g in range(SUBS):
                @pl.when(j > t)
                def _():
                    sum_hop(0, j, c, g).wait_send()

                @pl.when(j < t)
                def _():
                    sum_hop(1, j, c, g).wait_send()
        return carry

    lax.fori_loop(0, n, sums_drain, 0)
    for c in range(CHUNKS):
        for p in peers:
            sq_copy(c, t, p).wait_send()
    for k in range(CHUNKS * SUBS):
        for i, q in enumerate(mates):
            kv_copy(k, s, i, q).wait_send()
            kv_copy(k, q, len(mates) + i, partner).wait_send()
        kv_copy(k, s, m - 1, partner).wait_send()
        enc_store(k).wait()
        for slot in range(m):
            for cp in store_kv(k, s, slot):
                cp.wait()


def write_kernel(pieces, *refs):
    count = (len(refs) - 2) // 3
    srcs, dsts, bufs = refs[:count], refs[count:2 * count], refs[2 * count:3 * count]
    isem, wsem = refs[3 * count:]
    loads, stores = [], []
    for i in range(count):
        size = srcs[i].shape[0] // pieces
        for k in range(pieces):
            r = pl.ds(k * size, size)
            loads.append(pltpu.make_async_copy(srcs[i].at[r], bufs[i].at[r], isem.at[i, k]))
            stores.append(pltpu.make_async_copy(bufs[i].at[r], dsts[i].at[r], wsem.at[i, k]))
    for load in loads:
        load.start()
    for load, store in zip(loads, stores):
        load.wait()
        store.start()
    for store in stores:
        store.wait()


def write_out(arrays):
    count, pieces = len(arrays), 2
    any_spec = pl.BlockSpec(memory_space=pl.ANY)
    return pl.pallas_call(
        functools.partial(write_kernel, pieces),
        out_shape=tuple(jax.ShapeDtypeStruct(a.shape, a.dtype) for a in arrays),
        in_specs=[any_spec] * count,
        out_specs=(any_spec,) * count,
        scratch_shapes=[pltpu.VMEM(a.shape, a.dtype) for a in arrays]
        + [pltpu.SemaphoreType.DMA((count, pieces))] * 2,
    )(*arrays)


def on_device(n, m, stream, ffn_gain, final_gain, w_gate, w_up, w_out, w_key, w_value):
    rows, feat = stream.shape
    width = n * feat
    ffc = w_gate.shape[1]
    kvc = w_key.shape[1]
    crow = rows // CHUNKS
    bf, f32 = jnp.bfloat16, jnp.float32
    dma = pltpu.SemaphoreType.DMA
    any_spec = pl.BlockSpec(memory_space=pl.ANY)
    vmem = pl.BlockSpec(memory_space=pltpu.VMEM)
    parts = CHUNKS * SUBS
    made = pl.pallas_call(
        functools.partial(block_kernel, n, m),
        out_shape=(
            jax.ShapeDtypeStruct((rows, feat), bf),
            jax.ShapeDtypeStruct((m * rows, kvc), bf),
            jax.ShapeDtypeStruct((m * rows, kvc), bf),
        ),
        in_specs=[any_spec, vmem, vmem] + [any_spec] * 5,
        out_specs=(any_spec,) * 3,
        scratch_shapes=[
            pltpu.VMEM((width, ffc), bf),
            pltpu.VMEM((width, ffc), bf),
            pltpu.VMEM((ffc, width), bf),
            pltpu.VMEM((width, kvc), bf),
            pltpu.VMEM((width, kvc), bf),
            pltpu.VMEM((n, rows, feat), bf),
            pltpu.VMEM((n, rows, feat), bf),
            pltpu.VMEM((n, rows, feat), bf),
            pltpu.VMEM((n, rows, feat), bf),
            pltpu.VMEM((n, rows, feat), bf),
            pltpu.VMEM((crow, ffc), f32),
            pltpu.VMEM((crow, ffc), f32),
            pltpu.VMEM((crow, ffc), bf),
            pltpu.VMEM((crow, feat), f32),
            pltpu.VMEM((CHUNKS, crow, feat), f32),
            pltpu.VMEM((CHUNKS, n, 8, crow), f32),
            pltpu.VMEM((crow, kvc), f32),
            pltpu.VMEM((crow, kvc), f32),
            pltpu.VMEM((crow, 1), f32),
            pltpu.VMEM((crow, 1), f32),
            pltpu.VMEM((rows, feat), bf),
            pltpu.VMEM((m, parts, 2, crow // SUBS, kvc), bf),
            dma((5, n)),
            dma((CHUNKS,)),
            dma((2, n, parts)),
            dma((n, parts)),
            dma((n, parts)),
            dma((2, n, parts)),
            dma((2, n, parts)),
            dma((n, parts)),
            dma((CHUNKS, n)),
            dma((CHUNKS, n)),
            dma((m, parts)),
            dma((m, parts)),
            dma((2, m + 1, parts)),
        ],
        compiler_params=pltpu.CompilerParams(
            collective_id=0, has_side_effects=True, vmem_limit_bytes=67000000
        ),
    )(
        stream,
        ffn_gain.reshape(1, width),
        final_gain.reshape(1, width),
        w_gate, w_up, w_out, w_key, w_value,
    )
    return write_out(made)


def solution(mesh):
    placed = (
        P(("groups", "seq"), "tensor"),
        P(),
        P(),
        P(None, "tensor"),
        P(None, "tensor"),
        P("tensor", None),
        P(None, "tensor"),
        P(None, "tensor"),
    )
    return jax.shard_map(
        functools.partial(on_device, mesh.shape["tensor"], mesh.shape["seq"]),
        mesh=mesh,
        in_specs=placed,
        out_specs=(P(("groups", "seq"), "tensor"), P("groups", "tensor"), P("groups", "tensor")),
        check_vma=False,
    )
```
